32 devices in a mesh: lat: 4 (over z), rad: 8 (over y, x, core).
Axes of the slice: x: 2, y: 2, z: 4, core: 2. Of those that a mesh axis runs over, the one named last changes fastest.
Arguments:
- positions: float32 [4096, 3, 128], P(('lat', 'rad')), may hold values from 0 to 1
- fields: bfloat16 [4096, 16, 128], P(('lat', 'rad')), may hold values from -6 to 6
- velocity: float32 [81, 8192], P(None, ('lat', 'rad')), may hold values from -3 to 3
- counts: int32 [32], P(('lat', 'rad')), may hold values from 1 to 128, as said below
- elements: int32 [3, 4096], P(None, ('lat', 'rad')), may hold values from 0 to 255
- routes: int32 [2, 4096], P(None, ('lat', 'rad')), may hold values from 0 to 239, as said below
Outputs:
- moved: float32 [7680, 3, 128], P(('lat', 'rad'))
- projected: float32 [27, 16, 8192], P(None, None, ('lat', 'rad'))
The draws below stay inside these ranges and needn't reach their ends.
Inputs may be any that keep to these rules, and one draw needn't show every extreme that they name: counts[d] is at most 128 and equals 128 on some device. Both rows code destinations as in the reference program. routes[0] differs between any two blocks of one device; routes[1] differs between any two blocks that routes[0] sends to the same device.
All inputs are finite; a program needn't handle non-finite values.
Results may differ from the reference program's by a relative error of at most 0.0003.
Values sent between devices are 32-bit elements; how exact they have to be, the bound alone decides.
A program may use at most 64 MiB of HBM per device.

```python
import jax
import jax.numpy as jnp
from jax import lax

BLOCK = 128
FIELDS = 16
MB = 128
NE = 256
CAP = 10
SLOTS = 240
BLOCKS = 4096
ELEMS = 8192
N_LAT = 4
N_RAD = 8
DEVICES = 32


def draw_counts(key, part):
    keys = jax.random.split(jax.random.fold_in(key, 11), 2)
    lowest = max(1, MB // 4)
    drawn = jax.random.randint(keys[0], (DEVICES,), lowest, MB + 1)
    fullest = jax.random.randint(keys[1], (), 0, DEVICES)
    return jnp.where(jnp.arange(DEVICES) == fullest, MB, drawn).astype(jnp.int32)


def shuffled(key, height, width):
    scores = jax.random.randint(key, (height, width), 0, 1 << 20) * width + jnp.arange(width)[None, :]
    return jnp.argsort(scores, axis=1).astype(jnp.int32)


def draw_routes(key, part):
    keys = jax.random.split(jax.random.fold_in(key, 23), 2)
    first_route = shuffled(keys[0], DEVICES, SLOTS)[:, :MB].reshape(-1)
    home = jnp.arange(DEVICES * MB, dtype=jnp.int32) // MB
    lat_step = first_route // (N_RAD * CAP)
    mid_rad = first_route // CAP % N_RAD
    mid_place = first_route % CAP
    middle = (home // N_RAD + lat_step - 1) % N_LAT * N_RAD + mid_rad
    arrival = (lat_step * N_RAD + home % N_RAD) * CAP + mid_place
    second_route = shuffled(keys[1], DEVICES, SLOTS)[middle, arrival]
    return jnp.stack([first_route, second_route]).astype(jnp.int32)


def set_ends(result, key, smallest, top_value):
    place = [jax.random.randint(jax.random.fold_in(key, axis), (), 0, length) for axis, length in enumerate(result.shape)]
    longest = result.shape.index(max(result.shape))
    next_to = place[:longest] + [(place[longest] + 1) % result.shape[longest]] + place[longest + 1:]
    return result.at[tuple(place)].set(smallest).at[tuple(next_to)].set(top_value)


def block_levels(key, shape, cuts, least, top_value):
    loudness = 1.0
    for position, blocks in cuts:
        steps = jax.random.uniform(jax.random.fold_in(jax.random.fold_in(key, 6), position), (blocks,), jnp.float32, least / len(cuts), top_value / len(cuts))
        loudness = loudness * jnp.repeat(jnp.exp(steps), shape[position] // blocks).reshape((-1,) + (1,) * (len(shape) - 1 - position))
    return loudness


def bell_draw(rng, dims, deviation, limit, pieces=(), kind=jnp.bfloat16):
    result = deviation * jax.random.normal(rng, dims, jnp.float32)
    if pieces:
        result = result * block_levels(rng, dims, pieces, -0.22, 0.18)
    return jnp.clip(result, -limit, limit).astype(kind)


def setup_inputs(seed: int = 0) -> dict:
    seeds = jax.random.split(jax.random.key(seed), 7)
    return {
        "positions": jnp.clip(1.0 * jax.random.uniform(seeds[0], (BLOCKS, 3, BLOCK), jnp.float32) ** block_levels(seeds[0], (BLOCKS, 3, BLOCK), ((0, 32),), -0.2, 0.2), 0.0, 1.0),
        "fields": bell_draw(seeds[1], (BLOCKS, FIELDS, BLOCK), 1.0, 6.0, ((0, 32),)),
        "velocity": bell_draw(seeds[2], (81, ELEMS), 0.5, 3.0, ((1, 32),), jnp.float32),
        "counts": draw_counts(jax.random.fold_in(seeds[6], 71), 0),
        "elements": set_ends(jax.random.randint(seeds[4], (3, BLOCKS), 0, NE), jax.random.fold_in(seeds[4], 1), 0, NE - 1).astype(jnp.int32),
        "routes": draw_routes(jax.random.fold_in(seeds[6], 71), 0),
    }


time_step = 0.4
exact = lax.Precision.HIGHEST


def lagrange(coord):
    first_node = 2.0 * (coord - 0.5) * (coord - 1.0)
    middle_node = -4.0 * coord * (coord - 1.0)
    last_node = 2.0 * coord * (coord - 0.5)
    return jnp.stack([first_node, middle_node, last_node], axis=0)


def basis(points):
    along_x = lagrange(points[:, 0, :])
    along_y = lagrange(points[:, 1, :])
    along_z = lagrange(points[:, 2, :])
    table = along_x[:, None, None] * along_y[None, :, None] * along_z[None, None, :]
    return jnp.moveaxis(table.reshape(27, points.shape[0], points.shape[2]), 0, 1)


def speed(columns, points):
    coefficients = columns.T.reshape(points.shape[0], 3, 27)
    return jnp.einsum("scn,snb->scb", coefficients, basis(points), precision=exact)


def reference(positions, fields, velocity, counts, elements, routes):
    devices = N_LAT * N_RAD
    total = positions.shape[0]
    width = positions.shape[2]
    order = jnp.arange(total, dtype=jnp.int32)
    home = order // MB
    valid = (order % MB) < counts[home]
    lat_step = routes[0] // (N_RAD * CAP)
    mid_rad = (routes[0] // CAP) % N_RAD
    mid_lat = (home // N_RAD + lat_step - 1) % N_LAT
    middle = mid_lat * N_RAD + mid_rad
    next_step = routes[1] // (N_RAD * CAP)
    final_rad = (routes[1] // CAP) % N_RAD
    final_place = routes[1] % CAP
    final = ((mid_lat + next_step - 1) % N_LAT) * N_RAD + final_rad
    out_rows = (final * SLOTS + (next_step * N_RAD + mid_rad) * CAP + final_place).astype(jnp.int32)
    start_cols = (home * NE + elements[0]).astype(jnp.int32)
    middle_cols = (middle * NE + elements[1]).astype(jnp.int32)
    final_cols = (final * NE + elements[2]).astype(jnp.int32)

    def advance(block_set):
        points, fractions, start, middle_col = block_set
        first_speed = speed(jnp.take(velocity, start, axis=1), points)
        midway = points + (0.5 * time_step) * first_speed
        landed = points + time_step * speed(jnp.take(velocity, middle_col, axis=1), midway)
        shapes = basis(landed)
        moments = jnp.einsum("snb,sfb->snf", shapes, fractions.astype(jnp.float32), precision=exact)
        return landed, moments, jnp.sum(shapes * shapes, axis=2)

    landed, moments, weights = lax.map(advance, (positions.reshape(devices, MB, 3, width), fields.reshape(devices, MB, fields.shape[1], width), start_cols.reshape(devices, MB), middle_cols.reshape(devices, MB)))
    landed = landed.reshape(total, 3, width)
    moments = moments.reshape(total, 27, fields.shape[1])
    weights = weights.reshape(total, 27)
    live = valid.astype(jnp.float32)
    moved = jnp.zeros((devices * SLOTS, 3, width), jnp.float32).at[out_rows].set(landed * live[:, None, None])
    totals = jax.ops.segment_sum(moments * live[:, None, None], final_cols, num_segments=devices * NE)
    summed = jax.ops.segment_sum(weights * live[:, None], final_cols, num_segments=devices * NE)
    projected = totals / (1.0 + summed[:, :, None])
    return moved, jnp.transpose(projected, (1, 2, 0))
```

```python
import functools

import jax
import jax.numpy as jnp
from jax import lax
from jax.experimental import pallas as pl
from jax.experimental.pallas import tpu as pltpu
from jax.sharding import PartitionSpec as P

time_step = 0.4
MESH = pl.DeviceIdType.MESH
LANES = 128


def round_up(x, by):
    return -(-x // by) * by


def split(x):
    high = x.astype(jnp.bfloat16)
    low = (x - high.astype(jnp.float32)).astype(jnp.bfloat16)
    return high, low


def dot(a, b, dims):
    return lax.dot_general(a, b, (dims, ((), ())), preferred_element_type=jnp.float32)


def lagrange(s):
    return (2.0 * (s - 0.5) * (s - 1.0), -4.0 * s * (s - 1.0), 2.0 * s * (s - 0.5))


def advance(points_in, coefficients, base, out, scale, group):
    markers = base.shape[1]

    def step(g, carry):
        rows = pl.ds(pl.multiple_of(g * group, group), group)
        lx = lagrange(points_in[0, rows, :])
        ly = lagrange(points_in[1, rows, :])
        lz = lagrange(points_in[2, rows, :])
        sums = [None] * 3
        for i in range(3):
            inner = [None] * 3
            for j in range(3):
                for c in range(3):
                    n = c * 27 + 9 * i + 3 * j
                    line = (
                        coefficients[n : n + 1, :] * lz[0]
                        + coefficients[n + 1 : n + 2, :] * lz[1]
                        + coefficients[n + 2 : n + 3, :] * lz[2]
                    ) * ly[j]
                    inner[c] = line if inner[c] is None else inner[c] + line
            for c in range(3):
                term = inner[c] * lx[i]
                sums[c] = term if sums[c] is None else sums[c] + term
        for c in range(3):
            out[c, rows, :] = base[c, rows, :] + scale * sums[c]
        return carry

    lax.fori_loop(0, markers // group, step, 0)


def trip(
    n_lat, n_rad, capacity, padded,
    pos, fld, vel, tags,
    final,
    coef, midway, landed, phi, table, request, asked, answer, answered, outgoing, arrived, onward,
    send_sem, recv_sem,
):
    lat, rad = lax.axis_index("lat"), lax.axis_index("rad")
    slots = 3 * n_rad
    places = slots * capacity
    markers, fields, blocks = fld.shape
    owned = vel.shape[1]
    chunks = outgoing.shape[1]

    def partner(k, q, back):
        by = (1 - k) if back else (k - 1)
        return lax.rem(lat + by + n_lat, n_lat), q

    barrier = pltpu.get_barrier_semaphore()
    for k in range(3):

        def greet(dq, carry, k=k):
            q = lax.rem(rad + dq, n_rad)
            pl.semaphore_signal(
                barrier, inc=1, device_id=partner(k, q, False), device_id_type=MESH
            )
            return carry

        lax.fori_loop(1 if k == 1 else 0, n_rad, greet, 0)

    def exchange(phase, source, target, size, back=False):
        for k in (0, 2, 1):

            def send(dq, carry, k=k):
                q = lax.rem(rad + dq, n_rad)
                pltpu.make_async_remote_copy(
                    src_ref=source.at[pl.ds((k * n_rad + q) * size, size)],
                    dst_ref=target.at[pl.ds((k * n_rad + rad) * size, size)],
                    send_sem=send_sem.at[phase],
                    recv_sem=recv_sem.at[phase],
                    device_id=partner(k, q, back),
                    device_id_type=MESH,
                ).start()
                return carry

            lax.fori_loop(1 if k == 1 else 0, n_rad, send, 0)
        own = pl.ds((n_rad + rad) * size, size)
        pltpu.make_async_copy(source.at[own], target.at[own], recv_sem.at[phase]).start()

    def await_arrivals(phase, target):
        pltpu.make_async_copy(target, target, recv_sem.at[phase]).wait()

    def await_sends(phase, source, size):
        part = source.at[pl.ds(0, (slots - 1) * size)]
        pltpu.make_async_copy(part, part, send_sem.at[phase]).wait()

    rows = slots * padded
    padded_rows = lax.broadcasted_iota(jnp.int32, (rows, blocks), 0)
    spread = (padded_rows == tags[3:4, :]).astype(jnp.float32).astype(jnp.bfloat16)
    wanted = (tags[1:2, :] + 1).astype(jnp.float32)
    column = lax.broadcasted_iota(jnp.int32, (LANES, blocks), 0)
    labels = jnp.where(column == 0, wanted, 0.0)
    request[...] = dot(spread, labels.astype(jnp.bfloat16), ((1,), (1,))).reshape(
        slots, padded, LANES
    )
    pl.semaphore_wait(barrier, slots - 1)
    exchange(0, request, asked, 1)

    vel_high, vel_low = split(vel[...])
    element = lax.broadcasted_iota(jnp.int32, (owned, blocks), 0)
    pick = (element == tags[0:1, :]).astype(jnp.float32).astype(jnp.bfloat16)
    coef[...] = dot(vel_high, pick, ((1,), (0,))) + dot(vel_low, pick, ((1,), (0,)))
    advance(pos, coef, pos, midway, 0.5 * time_step, 16)

    await_arrivals(0, asked)
    wish = asked[...].reshape(rows, LANES)[:, 0:1].astype(jnp.int32)
    pick = (lax.broadcasted_iota(jnp.int32, (rows, owned), 1) + 1 == wish)
    pick = pick.astype(jnp.float32).astype(jnp.bfloat16)
    answer[...] = (
        dot(pick, vel_high, ((1,), (1,))) + dot(pick, vel_low, ((1,), (1,)))
    ).reshape(slots, padded, LANES)
    exchange(1, answer, answered, 1, back=True)
    await_arrivals(1, answered)
    high, low = split(answered[...].reshape(rows, LANES))
    coef[...] = dot(high, spread, ((0,), (0,))) + dot(low, spread, ((0,), (0,)))
    advance(midway, coef, pos, landed, time_step, 16)

    group = 8

    def tabulate(g, sums):
        part = pl.ds(pl.multiple_of(g * group, group), group)
        lx = lagrange(landed[0, part, :])
        ly = lagrange(landed[1, part, :])
        lz = lagrange(landed[2, part, :])
        new = []
        for i in range(3):
            for j in range(3):
                xy = lx[i] * ly[j]
                for k in range(3):
                    value = xy * lz[k]
                    n = 9 * i + 3 * j + k
                    phi[n, part, :] = value
                    new.append(sums[n] + value * value)
        return tuple(new)

    zero = jnp.zeros((group, blocks), jnp.float32)
    squares = lax.fori_loop(0, markers // group, tabulate, (zero,) * 27)
    first = 3 * markers
    table[pl.ds(0, first), :] = landed[...].reshape(first, blocks)
    base = first + 27 * fields
    table[pl.ds(base, table.shape[0] - base), :] = jnp.zeros(
        (table.shape[0] - base, blocks), jnp.float32
    )
    for n in range(27):
        table[base + n : base + n + 1, :] = jnp.sum(squares[n], axis=0, keepdims=True)
    table[base + 27 : base + 28, :] = (tags[2:3, :] + 1).astype(jnp.float32)
    table[base + 28 : base + 29, :] = (tags[5:6, :] + 1).astype(jnp.float32)
    for i in range(3):

        def gather(g, sums, i=i):
            for s in range(8):
                m = g * 8 + s
                carried = fld[m]
                sums = tuple(
                    sums[j] + phi[9 * i + j, pl.ds(m, 1), :] * carried for j in range(9)
                )
            return sums

        zero = jnp.zeros((fields, blocks), jnp.float32)
        sums = lax.fori_loop(0, markers // 8, gather, (zero,) * 9)
        for j in range(9):
            start = first + (9 * i + j) * fields
            table[start : start + fields, :] = sums[j]

    place = lax.broadcasted_iota(jnp.int32, (places, blocks), 0)
    spread = (place == tags[4:5, :]).astype(jnp.float32).astype(jnp.bfloat16)
    for j in range(chunks):
        high, low = split(table[pl.ds(j * LANES, LANES), :])
        outgoing[:, j, :] = dot(spread, high, ((1,), (1,))) + dot(spread, low, ((1,), (1,)))
    exchange(2, outgoing, arrived, capacity)
    await_arrivals(2, arrived)

    where_to, lane = divmod(base + 28, LANES)
    target = arrived[:, where_to, :][:, lane : lane + 1].astype(jnp.int32)
    turn = lax.broadcasted_iota(jnp.int32, (places, places), 1) + 1 == target
    turn = turn.astype(jnp.float32).T.astype(jnp.bfloat16)
    for j in range(chunks):
        high, low = split(arrived[:, j, :])
        onward[:, j, :] = dot(turn, high, ((1,), (0,))) + dot(turn, low, ((1,), (0,)))
    exchange(3, onward, final, capacity)
    await_arrivals(3, final)
    await_sends(0, request, 1)
    await_sends(1, answer, 1)
    await_sends(2, outgoing, capacity)
    await_sends(3, onward, capacity)


def settle(fields, markers, final, moved, projected):
    places = final.shape[0]
    owned = projected.shape[2]
    first = 3 * markers // LANES
    base = 27 * fields
    chunks = final.shape[1]
    moved[...] = final[:, 0:3, :]
    at, lane = divmod(3 * markers + base + 27, LANES)
    element = final[:, at, :][:, lane : lane + 1].astype(jnp.int32)
    hits = lax.broadcasted_iota(jnp.int32, (places, owned), 1) + 1 == element
    hits = hits.astype(jnp.float32).astype(jnp.bfloat16)
    sums = []
    for j in range(first, chunks):
        high, low = split(final[:, j, :].T)
        sums.append(dot(high, hits, ((1,), (0,))) + dot(low, hits, ((1,), (0,))))
    sums = jnp.concatenate(sums, axis=0)
    inverse = 1.0 / (1.0 + sums[base : base + 27, :])
    for n in range(27):
        projected[n] = sums[n * fields : (n + 1) * fields, :] * inverse[n : n + 1, :]


def per_device(n_lat, n_rad, positions, fields, velocity, counts, elements, routes):
    blocks, _, markers = positions.shape
    n_fields = fields.shape[1]
    capacity = max(1, 2 * blocks // (3 * n_rad))
    slots = 3 * n_rad
    places = slots * capacity
    padded = round_up(capacity, 8)
    owned = velocity.shape[1]
    chunks = round_up(3 * markers + 27 * n_fields + 29, LANES) // LANES
    live = jnp.arange(blocks, dtype=jnp.int32) < counts[0]
    wide = jnp.where(live, routes[0] // capacity * padded + routes[0] % capacity, -1)
    tags = jnp.concatenate(
        [elements, wide[None], jnp.where(live, routes[0], -1)[None], routes[1:2],
         jnp.zeros((2, blocks), jnp.int32)], axis=0
    )
    pos = jnp.transpose(positions, (1, 2, 0))
    fld = jnp.transpose(fields.astype(jnp.float32), (2, 1, 0))
    vel = jnp.pad(velocity, ((0, LANES - velocity.shape[0]), (0, 0)))
    f32 = jnp.float32
    vmem = pl.BlockSpec(memory_space=pltpu.VMEM)
    small = pltpu.VMEM((slots, padded, LANES), f32)
    large = pltpu.VMEM((places, chunks, LANES), f32)
    final = pl.pallas_call(
        functools.partial(trip, n_lat, n_rad, capacity, padded),
        out_shape=jax.ShapeDtypeStruct((places, chunks, LANES), f32),
        in_specs=[vmem] * 4,
        out_specs=vmem,
        scratch_shapes=[
            pltpu.VMEM((LANES, blocks), f32),
            pltpu.VMEM((3, markers, blocks), f32),
            pltpu.VMEM((3, markers, blocks), f32),
            pltpu.VMEM((27, markers, blocks), f32),
            pltpu.VMEM((chunks * LANES, blocks), f32),
            small, small, small, small,
            large, large, large,
            pltpu.SemaphoreType.DMA((4,)),
            pltpu.SemaphoreType.DMA((4,)),
        ],
        compiler_params=pltpu.CompilerParams(collective_id=0, has_side_effects=True),
        name="trip",
    )(pos, fld, vel, tags)
    return pl.pallas_call(
        functools.partial(settle, n_fields, markers),
        out_shape=(
            jax.ShapeDtypeStruct((places, 3, markers), f32),
            jax.ShapeDtypeStruct((27, n_fields, owned), f32),
        ),
        in_specs=[vmem],
        out_specs=(vmem, vmem),
        name="settle",
    )(final)


def solution(mesh):
    in_specs = (
        P(("lat", "rad"), None, None),
        P(("lat", "rad"), None, None),
        P(None, ("lat", "rad")),
        P(("lat", "rad")),
        P(None, ("lat", "rad")),
        P(None, ("lat", "rad")),
    )
    out_specs = (P(("lat", "rad"), None, None), P(None, None, ("lat", "rad")))
    return jax.shard_map(
        functools.partial(per_device, mesh.shape["lat"], mesh.shape["rad"]),
        mesh=mesh, in_specs=in_specs, out_specs=out_specs, check_vma=False,
    )
```

```python
import functools

import jax
import jax.numpy as jnp
from jax import lax
from jax.experimental import pallas as pl
from jax.experimental.pallas import tpu as pltpu
from jax.sharding import PartitionSpec as P

time_step = 0.4
MESH = pl.DeviceIdType.MESH
LANES = 128


def round_up(x, by):
    return -(-x // by) * by


def split(x):
    high = x.astype(jnp.bfloat16)
    low = (x - high.astype(jnp.float32)).astype(jnp.bfloat16)
    return high, low


def dot(a, b, dims):
    return lax.dot_general(a, b, (dims, ((), ())), preferred_element_type=jnp.float32)


def lagrange(s):
    return (2.0 * (s - 0.5) * (s - 1.0), -4.0 * s * (s - 1.0), 2.0 * s * (s - 0.5))


def advance(points_in, coefficients, base, out, scale, group):
    markers = base.shape[1]

    def step(g, carry):
        rows = pl.ds(pl.multiple_of(g * group, group), group)
        lx = lagrange(points_in[0, rows, :])
        ly = lagrange(points_in[1, rows, :])
        lz = lagrange(points_in[2, rows, :])
        sums = [None] * 3
        for i in range(3):
            inner = [None] * 3
            for j in range(3):
                for c in range(3):
                    n = c * 27 + 9 * i + 3 * j
                    line = (
                        coefficients[n : n + 1, :] * lz[0]
                        + coefficients[n + 1 : n + 2, :] * lz[1]
                        + coefficients[n + 2 : n + 3, :] * lz[2]
                    ) * ly[j]
                    inner[c] = line if inner[c] is None else inner[c] + line
            for c in range(3):
                term = inner[c] * lx[i]
                sums[c] = term if sums[c] is None else sums[c] + term
        for c in range(3):
            out[c, rows, :] = base[c, rows, :] + scale * sums[c]
        return carry

    lax.fori_loop(0, markers // group, step, 0)


def trip(
    n_lat, n_rad, capacity,
    counts, pos, vel, elements, routes, fld,
    *rest,
):
    final, rest = rest[:3], rest[3:]
    raw, wide, carried, start_points, coef, midway, landed, phi, table = rest[:9]
    request, asked, answer, answered = rest[9:13]
    outgoing, arrived, onward = rest[13:16], rest[16:19], rest[19:22]
    load_sem, send_sem, recv_sem = rest[22:]
    lat, rad = lax.axis_index("lat"), lax.axis_index("rad")
    slots = 3 * n_rad
    places = slots * capacity
    blocks, fields, markers = fld.shape
    owned = vel.shape[1]
    bf16, f32 = jnp.bfloat16, jnp.float32
    load = pltpu.make_async_copy(fld, raw, load_sem)
    load.start()

    def partner(k, q, back):
        by = (1 - k) if back else (k - 1)
        return lax.rem(lat + by + n_lat, n_lat), q

    barrier = pltpu.get_barrier_semaphore()
    for k in range(3):

        def greet(dq, carry, k=k):
            q = lax.rem(rad + dq, n_rad)
            pl.semaphore_signal(
                barrier, inc=1, device_id=partner(k, q, False), device_id_type=MESH
            )
            return carry

        lax.fori_loop(1 if k == 1 else 0, n_rad, greet, 0)

    def exchange(phase, source, target, size, back=False):
        for k in (0, 2, 1):

            def send(dq, carry, k=k):
                q = lax.rem(rad + dq, n_rad)
                pltpu.make_async_remote_copy(
                    src_ref=source.at[pl.ds((k * n_rad + q) * size, size)],
                    dst_ref=target.at[pl.ds((k * n_rad + rad) * size, size)],
                    send_sem=send_sem.at[phase],
                    recv_sem=recv_sem.at[phase],
                    device_id=partner(k, q, back),
                    device_id_type=MESH,
                ).start()
                return carry

            lax.fori_loop(1 if k == 1 else 0, n_rad, send, 0)
        own = pl.ds((n_rad + rad) * size, size)
        pltpu.make_async_copy(source.at[own], target.at[own], recv_sem.at[phase]).start()

    def await_arrivals(phase, target):
        pltpu.make_async_copy(target, target, recv_sem.at[phase]).wait()

    def await_sends(phase, source, size):
        part = source.at[pl.ds(0, (slots - 1) * size)]
        pltpu.make_async_copy(part, part, send_sem.at[phase]).wait()

    def iota(shape, axis):
        return lax.broadcasted_iota(jnp.int32, shape, axis)

    def slot_of(place):
        return jnp.floor((place.astype(f32) + 0.5) * (1.0 / capacity)).astype(jnp.int32)

    def mask(condition):
        return condition.astype(f32).astype(bf16)

    route = jnp.where(iota((1, blocks), 1) < counts[0], routes[0:1, :], -1)
    slot = slot_of(route)
    sent_to = iota((slots, blocks), 0) == slot
    within = mask(iota((LANES, blocks), 0) == route - slot * capacity)
    for row, label in enumerate((elements[1:2, :], routes[1:2, :])):
        marked = jnp.where(sent_to, (label + 1).astype(f32), 0.0).astype(bf16)
        request[:, row, :] = dot(marked, within, ((1,), (1,)))
    pl.semaphore_wait(barrier, slots - 1)
    exchange(0, request, asked, 1)

    for c in range(3):
        start_points[c] = pos[c].T
    vel_high, vel_low = split(vel[...])
    pick = mask(iota((owned, blocks), 0) == elements[0:1, :])
    coef[...] = dot(vel_high, pick, ((1,), (0,))) + dot(vel_low, pick, ((1,), (0,)))
    advance(start_points, coef, start_points, midway, 0.5 * time_step, 16)
    spread = mask(iota((places, blocks), 0) == route)

    own_slot = slot_of(iota((places, slots), 0))
    by_slot = mask(own_slot == iota((places, slots), 1))
    lane = iota((places, LANES), 0) - slot_of(iota((places, LANES), 0)) * capacity
    by_lane = lane == iota((places, LANES), 1)

    def label_column(row):
        lines = dot(by_slot, asked[:, row, :].astype(bf16), ((1,), (0,)))
        return jnp.sum(jnp.where(by_lane, lines, 0.0), axis=1, keepdims=True).astype(jnp.int32)

    await_arrivals(0, asked)
    pick = mask(iota((places, owned), 1) + 1 == label_column(0))
    answer[:, 0, 0 : vel.shape[0]] = dot(pick, vel_high, ((1,), (1,))) + dot(
        pick, vel_low, ((1,), (1,))
    )
    answer[:, 0, vel.shape[0] :] = jnp.zeros((places, LANES - vel.shape[0]), f32)
    exchange(1, answer, answered, capacity, back=True)
    turn = (iota((places, places), 1) + 1 == label_column(1)).astype(f32).T.astype(bf16)
    load.wait()
    wide[...] = raw[...].astype(f32)
    for f in range(fields):
        carried[:, f, :] = wide[:, f, :].T
    await_arrivals(1, answered)
    high, low = split(answered[:, 0, 0 : vel.shape[0]])
    coef[...] = dot(high, spread, ((0,), (0,))) + dot(low, spread, ((0,), (0,)))
    advance(midway, coef, start_points, landed, time_step, 16)

    group = 8

    def tabulate(g, sums):
        part = pl.ds(pl.multiple_of(g * group, group), group)
        lx = lagrange(landed[0, part, :])
        ly = lagrange(landed[1, part, :])
        lz = lagrange(landed[2, part, :])
        new = []
        for i in range(3):
            for j in range(3):
                xy = lx[i] * ly[j]
                for k in range(3):
                    value = xy * lz[k]
                    n = 9 * i + 3 * j + k
                    phi[n, part, :] = value
                    new.append(sums[n] + value * value)
        return tuple(new)

    zero = jnp.zeros((group, blocks), f32)
    squares = lax.fori_loop(0, markers // group, tabulate, (zero,) * 27)

    def moments(nodes, first):
        def gather(g, sums):
            for s in range(8):
                m = g * 8 + s
                values = carried[m]
                sums = tuple(
                    total + phi[n, pl.ds(m, 1), :] * values for total, n in zip(sums, nodes)
                )
            return sums

        zero = jnp.zeros((fields, blocks), f32)
        sums = lax.fori_loop(0, markers // 8, gather, (zero,) * len(nodes))
        for index, total in enumerate(sums):
            table[first + index * fields : first + (index + 1) * fields, :] = total

    def put(buffer, j, rows):
        high, low = split(rows)
        buffer[:, j, :] = dot(spread, high, ((1,), (1,))) + dot(spread, low, ((1,), (1,)))

    per_row = LANES // fields
    full = 27 // per_row
    last = tuple(range(full * per_row, 27))
    moments(last, 0)
    base = len(last) * fields
    table[base:LANES, :] = jnp.zeros((LANES - base, blocks), f32)
    for n in range(27):
        table[base + n : base + n + 1, :] = jnp.sum(squares[n], axis=0, keepdims=True)
    table[base + 27 : base + 28, :] = (elements[2:3, :] + 1).astype(f32)
    for c in range(3):
        put(outgoing[0], c, landed[c])
    put(outgoing[0], 3, table[0:LANES, :])
    exchange(2, outgoing[0], arrived[0], capacity)
    node = 0
    for part in (1, 2):
        for j in range(outgoing[part].shape[1]):
            moments(tuple(range(node, node + per_row)), 0)
            node += per_row
            put(outgoing[part], j, table[0:LANES, :])
        exchange(2 + part, outgoing[part], arrived[part], capacity)

    for part in range(3):
        await_arrivals(2 + part, arrived[part])
        for j in range(arrived[part].shape[1]):
            high, low = split(arrived[part][:, j, :])
            onward[part][:, j, :] = dot(turn, high, ((1,), (0,))) + dot(turn, low, ((1,), (0,)))
        exchange(5 + part, onward[part], final[part], capacity)
    for part in range(3):
        await_arrivals(5 + part, final[part])
    await_sends(0, request, 1)
    await_sends(1, answer, capacity)
    for part in range(3):
        await_sends(2 + part, outgoing[part], capacity)
        await_sends(5 + part, onward[part], capacity)


def settle(fields, first, second, third, moved, projected):
    places = first.shape[0]
    owned = projected.shape[2]
    per_row = LANES // fields
    base = (27 - 27 // per_row * per_row) * fields
    for c in range(3):
        moved[c] = first[:, c, :]
    element = first[:, 3, :][:, base + 27 : base + 28].astype(jnp.int32)
    hits = lax.broadcasted_iota(jnp.int32, (places, owned), 1) + 1 == element
    hits = hits.astype(jnp.float32).astype(jnp.bfloat16)

    def total(lines):
        high, low = split(lines.T)
        return dot(high, hits, ((1,), (0,))) + dot(low, hits, ((1,), (0,)))

    tail = total(first[:, 3, :])
    inverse = 1.0 / (1.0 + tail[base : base + 27, :])
    node = 0
    for part in (second, third):
        for j in range(part.shape[1]):
            sums = total(part[:, j, :])
            for n in range(per_row):
                projected[node] = sums[n * fields : (n + 1) * fields, :] * inverse[node : node + 1, :]
                node += 1
    for n in range(27 - node):
        projected[node + n] = (
            tail[n * fields : (n + 1) * fields, :] * inverse[node + n : node + n + 1, :]
        )


def per_device(n_lat, n_rad, positions, fields, velocity, counts, elements, routes):
    blocks, _, markers = positions.shape
    n_fields = fields.shape[1]
    capacity = max(1, 2 * blocks // (3 * n_rad))
    slots = 3 * n_rad
    places = slots * capacity
    owned = velocity.shape[1]
    full = 27 * n_fields // LANES
    f32 = jnp.float32
    vmem = pl.BlockSpec(memory_space=pltpu.VMEM)
    small = pltpu.VMEM((slots, 2, LANES), f32)
    line = pltpu.VMEM((places, 1, LANES), f32)
    points = pltpu.VMEM((3, markers, blocks), f32)
    shapes = [(places, 4, LANES), (places, full - 1, LANES), (places, 1, LANES)]
    parts = [pltpu.VMEM(shape, f32) for shape in shapes]
    final = pl.pallas_call(
        functools.partial(trip, n_lat, n_rad, capacity),
        out_shape=[jax.ShapeDtypeStruct(shape, f32) for shape in shapes],
        in_specs=[pl.BlockSpec(memory_space=pltpu.SMEM)] + [vmem] * 4
        + [pl.BlockSpec(memory_space=pl.ANY)],
        out_specs=[vmem] * 3,
        scratch_shapes=[
            pltpu.VMEM(fields.shape, fields.dtype),
            pltpu.VMEM(fields.shape, f32),
            pltpu.VMEM((markers, n_fields, blocks), f32),
            points,
            pltpu.VMEM((velocity.shape[0], blocks), f32),
            points,
            points,
            pltpu.VMEM((27, markers, blocks), f32),
            pltpu.VMEM((LANES, blocks), f32),
            small, small, line, line,
            *parts, *parts, *parts,
            pltpu.SemaphoreType.DMA,
            pltpu.SemaphoreType.DMA((8,)),
            pltpu.SemaphoreType.DMA((8,)),
        ],
        compiler_params=pltpu.CompilerParams(collective_id=0, has_side_effects=True),
        name="trip",
    )(counts, jnp.transpose(positions, (1, 0, 2)), velocity, elements, routes, fields)
    moved, projected = pl.pallas_call(
        functools.partial(settle, n_fields),
        out_shape=(
            jax.ShapeDtypeStruct((3, places, markers), f32),
            jax.ShapeDtypeStruct((27, n_fields, owned), f32),
        ),
        in_specs=[vmem] * 3,
        out_specs=(vmem, vmem),
        name="settle",
    )(*final)
    return jnp.transpose(moved, (1, 0, 2)), projected


def solution(mesh):
    in_specs = (
        P(("lat", "rad"), None, None),
        P(("lat", "rad"), None, None),
        P(None, ("lat", "rad")),
        P(("lat", "rad")),
        P(None, ("lat", "rad")),
        P(None, ("lat", "rad")),
    )
    out_specs = (P(("lat", "rad"), None, None), P(None, None, ("lat", "rad")))
    return jax.shard_map(
        functools.partial(per_device, mesh.shape["lat"], mesh.shape["rad"]),
        mesh=mesh, in_specs=in_specs, out_specs=out_specs, check_vma=False,
    )
```

```python
import functools

import jax
import jax.numpy as jnp
from jax import lax
from jax.experimental import pallas as pl
from jax.experimental.pallas import tpu as pltpu
from jax.sharding import PartitionSpec as P

time_step = 0.4
MESH = pl.DeviceIdType.MESH
LANES = 128


def round_up(x, by):
    return -(-x // by) * by


def split(x):
    high = x.astype(jnp.bfloat16)
    low = (x - high.astype(jnp.float32)).astype(jnp.bfloat16)
    return high, low


def dot(a, b, dims):
    return lax.dot_general(a, b, (dims, ((), ())), preferred_element_type=jnp.float32)


def lagrange(s):
    return (2.0 * (s - 0.5) * (s - 1.0), -4.0 * s * (s - 1.0), 2.0 * s * (s - 0.5))


def advance(points_in, coefficients, base, out, scale, group):
    markers = base.shape[1]

    def step(g, carry):
        rows = pl.ds(pl.multiple_of(g * group, group), group)
        lx = lagrange(points_in[0, rows, :])
        ly = lagrange(points_in[1, rows, :])
        lz = lagrange(points_in[2, rows, :])
        sums = [None] * 3
        for i in range(3):
            inner = [None] * 3
            for j in range(3):
                for c in range(3):
                    n = c * 27 + 9 * i + 3 * j
                    line = (
                        coefficients[n : n + 1, :] * lz[0]
                        + coefficients[n + 1 : n + 2, :] * lz[1]
                        + coefficients[n + 2 : n + 3, :] * lz[2]
                    ) * ly[j]
                    inner[c] = line if inner[c] is None else inner[c] + line
            for c in range(3):
                term = inner[c] * lx[i]
                sums[c] = term if sums[c] is None else sums[c] + term
        for c in range(3):
            out[c, rows, :] = base[c, rows, :] + scale * sums[c]
        return carry

    lax.fori_loop(0, markers // group, step, 0)


def trip(
    n_lat, n_rad, capacity,
    counts, pos, vel, elements, routes, fld,
    *rest,
):
    final, rest = rest[:3], rest[3:]
    raw, wide, carried, start_points, coef, midway, landed, phi, table = rest[:9]
    request, asked, answer, answered = rest[9:13]
    outgoing, arrived, onward = rest[13:16], rest[16:19], rest[19:22]
    load_sem, send_sem, recv_sem = rest[22:]
    lat, rad = lax.axis_index("lat"), lax.axis_index("rad")
    slots = 3 * n_rad
    places = slots * capacity
    blocks, fields, markers = fld.shape
    owned = vel.shape[1]
    bf16, f32 = jnp.bfloat16, jnp.float32
    load = pltpu.make_async_copy(fld, raw, load_sem)
    load.start()

    def partner(k, q, back):
        by = (1 - k) if back else (k - 1)
        return lax.rem(lat + by + n_lat, n_lat), q

    barrier = pltpu.get_barrier_semaphore()
    for k in range(3):

        def greet(dq, carry, k=k):
            q = lax.rem(rad + dq, n_rad)
            pl.semaphore_signal(
                barrier, inc=1, device_id=partner(k, q, False), device_id_type=MESH
            )
            return carry

        lax.fori_loop(1 if k == 1 else 0, n_rad, greet, 0)

    def exchange(phase, source, target, size, back=False):
        for k in (0, 2, 1):

            def send(dq, carry, k=k):
                q = lax.rem(rad + dq, n_rad)
                pltpu.make_async_remote_copy(
                    src_ref=source.at[pl.ds((k * n_rad + q) * size, size)],
                    dst_ref=target.at[pl.ds((k * n_rad + rad) * size, size)],
                    send_sem=send_sem.at[phase],
                    recv_sem=recv_sem.at[phase],
                    device_id=partner(k, q, back),
                    device_id_type=MESH,
                ).start()
                return carry

            lax.fori_loop(1 if k == 1 else 0, n_rad, send, 0)
        own = pl.ds((n_rad + rad) * size, size)
        pltpu.make_async_copy(source.at[own], target.at[own], recv_sem.at[phase]).start()

    def await_arrivals(phase, target):
        pltpu.make_async_copy(target, target, recv_sem.at[phase]).wait()

    def await_sends(phase, source, size):
        part = source.at[pl.ds(0, (slots - 1) * size)]
        pltpu.make_async_copy(part, part, send_sem.at[phase]).wait()

    def iota(shape, axis):
        return lax.broadcasted_iota(jnp.int32, shape, axis)

    def slot_of(place):
        return jnp.floor((place.astype(f32) + 0.5) * (1.0 / capacity)).astype(jnp.int32)

    def mask(condition):
        return condition.astype(f32).astype(bf16)

    route = jnp.where(iota((1, blocks), 1) < counts[0], routes[0:1, :], -1)
    slot = slot_of(route)
    sent_to = iota((slots, blocks), 0) == slot
    within = mask(iota((LANES, blocks), 0) == route - slot * capacity)
    for row, label in enumerate((elements[1:2, :], routes[1:2, :])):
        marked = jnp.where(sent_to, (label + 1).astype(f32), 0.0).astype(bf16)
        request[:, row, :] = dot(marked, within, ((1,), (1,)))
    pl.semaphore_wait(barrier, slots - 1)
    exchange(0, request, asked, 1)

    for c in range(3):
        start_points[c] = pos[c].T
    vel_high, vel_low = split(vel[...])
    pick = mask(iota((owned, blocks), 0) == elements[0:1, :])
    coef[...] = dot(vel_high, pick, ((1,), (0,))) + dot(vel_low, pick, ((1,), (0,)))
    advance(start_points, coef, start_points, midway, 0.5 * time_step, 16)
    spread = mask(iota((places, blocks), 0) == route)

    def put(buffer, j, rows):
        high, low = split(rows)
        buffer[:, j, :] = dot(spread, high, ((1,), (1,))) + dot(spread, low, ((1,), (1,)))

    own_slot = slot_of(iota((places, slots), 0))
    by_slot = mask(own_slot == iota((places, slots), 1))
    lane = iota((places, LANES), 0) - slot_of(iota((places, LANES), 0)) * capacity
    by_lane = lane == iota((places, LANES), 1)

    def label_column(row):
        lines = dot(by_slot, asked[:, row, :].astype(bf16), ((1,), (0,)))
        return jnp.sum(jnp.where(by_lane, lines, 0.0), axis=1, keepdims=True).astype(jnp.int32)

    await_arrivals(0, asked)
    pick = mask(iota((places, owned), 1) + 1 == label_column(0))
    answer[:, 0, 0 : vel.shape[0]] = dot(pick, vel_high, ((1,), (1,))) + dot(
        pick, vel_low, ((1,), (1,))
    )
    answer[:, 0, vel.shape[0] :] = jnp.zeros((places, LANES - vel.shape[0]), f32)
    exchange(1, answer, answered, capacity, back=True)
    turn = (iota((places, places), 1) + 1 == label_column(1)).astype(f32).T.astype(bf16)
    load.wait()
    wide[...] = raw[...].astype(f32)
    for f in range(fields):
        carried[:, f, :] = wide[:, f, :].T
    await_arrivals(1, answered)
    high, low = split(answered[:, 0, 0 : vel.shape[0]])
    coef[...] = dot(high, spread, ((0,), (0,))) + dot(low, spread, ((0,), (0,)))
    advance(midway, coef, start_points, landed, time_step, 16)

    for c in range(2):
        put(outgoing[0], c, landed[c])
    exchange(2, outgoing[0], arrived[0], capacity)
    put(outgoing[1], 0, landed[2])
    exchange(3, outgoing[1], arrived[1], capacity)

    group = 8

    def tabulate(g, sums):
        part = pl.ds(pl.multiple_of(g * group, group), group)
        lx = lagrange(landed[0, part, :])
        ly = lagrange(landed[1, part, :])
        lz = lagrange(landed[2, part, :])
        new = []
        for i in range(3):
            for j in range(3):
                xy = lx[i] * ly[j]
                for k in range(3):
                    value = xy * lz[k]
                    n = 9 * i + 3 * j + k
                    phi[n, part, :] = value
                    new.append(sums[n] + value * value)
        return tuple(new)

    zero = jnp.zeros((group, blocks), f32)
    squares = lax.fori_loop(0, markers // group, tabulate, (zero,) * 27)

    def moments(nodes, first):
        def gather(g, sums):
            for s in range(8):
                m = g * 8 + s
                values = carried[m]
                sums = tuple(
                    total + phi[n, pl.ds(m, 1), :] * values for total, n in zip(sums, nodes)
                )
            return sums

        zero = jnp.zeros((fields, blocks), f32)
        sums = lax.fori_loop(0, markers // 8, gather, (zero,) * len(nodes))
        for index, total in enumerate(sums):
            table[first + index * fields : first + (index + 1) * fields, :] = total

    per_row = LANES // fields
    full = 27 // per_row
    last = tuple(range(full * per_row, 27))
    moments(last, 0)
    base = len(last) * fields
    table[base:LANES, :] = jnp.zeros((LANES - base, blocks), f32)
    for n in range(27):
        table[base + n : base + n + 1, :] = jnp.sum(squares[n], axis=0, keepdims=True)
    table[base + 27 : base + 28, :] = (elements[2:3, :] + 1).astype(f32)
    put(outgoing[2], full, table[0:LANES, :])
    for j in range(full):
        moments(tuple(range(j * per_row, (j + 1) * per_row)), 0)
        put(outgoing[2], j, table[0:LANES, :])
    exchange(4, outgoing[2], arrived[2], capacity)

    for part in range(3):
        await_arrivals(2 + part, arrived[part])
        for j in range(arrived[part].shape[1]):
            high, low = split(arrived[part][:, j, :])
            onward[part][:, j, :] = dot(turn, high, ((1,), (0,))) + dot(turn, low, ((1,), (0,)))
        exchange(5 + part, onward[part], final[part], capacity)
    for part in range(3):
        await_arrivals(5 + part, final[part])
    await_sends(0, request, 1)
    await_sends(1, answer, capacity)
    for part in range(3):
        await_sends(2 + part, outgoing[part], capacity)
        await_sends(5 + part, onward[part], capacity)


def settle(fields, first, second, third, moved, projected):
    places = first.shape[0]
    owned = projected.shape[2]
    per_row = LANES // fields
    base = (27 - 27 // per_row * per_row) * fields
    moved[0] = first[:, 0, :]
    moved[1] = first[:, 1, :]
    moved[2] = second[:, 0, :]
    full = third.shape[1] - 1
    element = third[:, full, :][:, base + 27 : base + 28].astype(jnp.int32)
    hits = lax.broadcasted_iota(jnp.int32, (places, owned), 1) + 1 == element
    hits = hits.astype(jnp.float32).astype(jnp.bfloat16)

    def total(lines):
        high, low = split(lines.T)
        return dot(high, hits, ((1,), (0,))) + dot(low, hits, ((1,), (0,)))

    tail = total(third[:, full, :])
    inverse = 1.0 / (1.0 + tail[base : base + 27, :])
    node = 0
    for j in range(full):
        sums = total(third[:, j, :])
        for n in range(per_row):
            projected[node] = sums[n * fields : (n + 1) * fields, :] * inverse[node : node + 1, :]
            node += 1
    for n in range(27 - node):
        projected[node + n] = (
            tail[n * fields : (n + 1) * fields, :] * inverse[node + n : node + n + 1, :]
        )


def per_device(n_lat, n_rad, positions, fields, velocity, counts, elements, routes):
    blocks, _, markers = positions.shape
    n_fields = fields.shape[1]
    capacity = max(1, 2 * blocks // (3 * n_rad))
    slots = 3 * n_rad
    places = slots * capacity
    owned = velocity.shape[1]
    full = 27 * n_fields // LANES
    f32 = jnp.float32
    vmem = pl.BlockSpec(memory_space=pltpu.VMEM)
    small = pltpu.VMEM((slots, 2, LANES), f32)
    line = pltpu.VMEM((places, 1, LANES), f32)
    points = pltpu.VMEM((3, markers, blocks), f32)
    shapes = [(places, 2, LANES), (places, 1, LANES), (places, full + 1, LANES)]
    parts = [pltpu.VMEM(shape, f32) for shape in shapes]
    final = pl.pallas_call(
        functools.partial(trip, n_lat, n_rad, capacity),
        out_shape=[jax.ShapeDtypeStruct(shape, f32) for shape in shapes],
        in_specs=[pl.BlockSpec(memory_space=pltpu.SMEM)] + [vmem] * 4
        + [pl.BlockSpec(memory_space=pl.ANY)],
        out_specs=[vmem] * 3,
        scratch_shapes=[
            pltpu.VMEM(fields.shape, fields.dtype),
            pltpu.VMEM(fields.shape, f32),
            pltpu.VMEM((markers, n_fields, blocks), f32),
            points,
            pltpu.VMEM((velocity.shape[0], blocks), f32),
            points,
            points,
            pltpu.VMEM((27, markers, blocks), f32),
            pltpu.VMEM((LANES, blocks), f32),
            small, small, line, line,
            *parts, *parts, *parts,
            pltpu.SemaphoreType.DMA,
            pltpu.SemaphoreType.DMA((8,)),
            pltpu.SemaphoreType.DMA((8,)),
        ],
        compiler_params=pltpu.CompilerParams(collective_id=0, has_side_effects=True),
        name="trip",
    )(counts, jnp.transpose(positions, (1, 0, 2)), velocity, elements, routes, fields)
    moved, projected = pl.pallas_call(
        functools.partial(settle, n_fields),
        out_shape=(
            jax.ShapeDtypeStruct((3, places, markers), f32),
            jax.ShapeDtypeStruct((27, n_fields, owned), f32),
        ),
        in_specs=[vmem] * 3,
        out_specs=(vmem, vmem),
        name="settle",
    )(*final)
    return jnp.transpose(moved, (1, 0, 2)), projected


def solution(mesh):
    in_specs = (
        P(("lat", "rad"), None, None),
        P(("lat", "rad"), None, None),
        P(None, ("lat", "rad")),
        P(("lat", "rad")),
        P(None, ("lat", "rad")),
        P(None, ("lat", "rad")),
    )
    out_specs = (P(("lat", "rad"), None, None), P(None, None, ("lat", "rad")))
    return jax.shard_map(
        functools.partial(per_device, mesh.shape["lat"], mesh.shape["rad"]),
        mesh=mesh, in_specs=in_specs, out_specs=out_specs, check_vma=False,
    )
```
